32 devices in a mesh: gx: 4 (over z), gy: 2 (over x), gz: 4 (over y, core).
Axes of the slice: x: 2, y: 2, z: 4, core: 2. Of those that a mesh axis runs over, the one named last changes fastest.
Arguments:
- start_potential: float32 [64, 256, 512], P('gx', 'gy', 'gz'), may hold values from -0.9 to 2.1
- permittivity: float32 [64, 256, 512], P('gx', 'gy', 'gz'), may hold values from 1 to 8
- screening: float32 [64, 256, 512], P('gx', 'gy', 'gz'), may hold values from 0.05 to 2
- source: float32 [64, 256, 512], P('gx', 'gy', 'gz'), may hold values from -12 to 12
Outputs:
- potential: float32 [64, 256, 512], P('gx', 'gy', 'gz')
- residual_rms: float32 [3], replicated
- induced_charge: float32 [3], replicated
The draws below stay inside these ranges and needn't reach their ends.
All inputs are finite; a program needn't handle non-finite values.
Results may differ from the reference program's by a relative error of at most 0.0003.
Values sent between devices are 32-bit elements; how exact they have to be, the bound alone decides.
No kernel may reach another device: no remote copies, remote signals or barrier semaphores. Data moves between devices by JAX's collectives and lax.ppermute only.
A program may use at most 64 MiB of HBM per device.

```python
import math
import jax
import jax.numpy as jnp

ITERS = 3
NX = 64
NY = 256
NZ = 512


def coordinate_ramp():
    first = (jnp.arange(NX, dtype=jnp.float32) + 0.5) / NX
    second = (jnp.arange(NY, dtype=jnp.float32) + 0.5) / NY
    third = (jnp.arange(NZ, dtype=jnp.float32) + 0.5) / NZ
    total = first[:, None, None] + second[None, :, None] + third[None, None, :]
    return 1.0 + 2.0 * total / 3.0


def draw_start_potential(key, part):
    key = jax.random.fold_in(key, 11)
    ramp = coordinate_ramp()
    noise = jnp.clip(jax.random.normal(key, (NX, NY, NZ), jnp.float32), -4.0, 4.0)
    return 0.3 * ramp + 0.3 * noise


def draw_source(key, part):
    key = jax.random.fold_in(key, 23)
    ramp = coordinate_ramp()
    noise = jnp.clip(jax.random.normal(key, (NX, NY, NZ), jnp.float32), -4.0, 4.0)
    return ramp * noise


def block_levels(rng, dims, pieces, smallest, high):
    level = 1.0
    for dim, blocks in pieces:
        steps = jax.random.uniform(jax.random.fold_in(jax.random.fold_in(rng, 6), dim), (blocks,), jnp.float32, smallest / len(pieces), high / len(pieces))
        level = level * jnp.repeat(jnp.exp(steps), dims[dim] // blocks).reshape((-1,) + (1,) * (len(dims) - 1 - dim))
    return level


def setup_inputs(seed: int = 0) -> dict:
    key_of = jax.random.split(jax.random.key(seed), 5)
    start_potential = draw_start_potential(jax.random.fold_in(key_of[4], 71), 0)
    permittivity = jnp.clip(jnp.exp(math.log(8.0) - 2.0794415 * jax.random.uniform(key_of[1], (NX, NY, NZ), jnp.float32) ** block_levels(key_of[1], (NX, NY, NZ), ((0, 4), (1, 2), (2, 4)), -0.2, 0.2)), 1.0, 8.0)
    screening = jnp.clip(jnp.exp(math.log(2.0) - 3.6888794 * jax.random.uniform(key_of[2], (NX, NY, NZ), jnp.float32) ** block_levels(key_of[2], (NX, NY, NZ), ((0, 4), (1, 2), (2, 4)), -0.2, 0.2)), 0.05, 2.0)
    source = draw_source(jax.random.fold_in(key_of[4], 71), 0)
    return {"start_potential": start_potential, "permittivity": permittivity, "screening": screening, "source": source}


def harmonic(left, right):
    total = left + right
    return 2.0 * left * right / jnp.where(total > 0, total, 1.0)

def neighbours(block):
    return [block[2:, 1:-1, 1:-1], block[:-2, 1:-1, 1:-1], block[1:-1, 2:, 1:-1], block[1:-1, :-2, 1:-1], block[1:-1, 1:-1, 2:], block[1:-1, 1:-1, :-2]]

def relax(padded, weights_pad, screening, source):
    center = padded[1:-1, 1:-1, 1:-1]
    middle = weights_pad[1:-1, 1:-1, 1:-1]
    flux = jnp.zeros_like(center)
    diagonal = jnp.zeros_like(center)
    for near, other in zip(neighbours(padded), neighbours(weights_pad)):
        weight = harmonic(middle, other)
        flux = flux + weight * (center - near)
        diagonal = diagonal + weight
    induced = screening * jnp.sinh(center)
    residual = source - flux - induced
    diagonal = diagonal + screening * jnp.cosh(center)
    return (center, residual, jnp.where(diagonal > 0, diagonal, 1.0), induced)

def reference(start_potential, permittivity, screening, source):
    cells = NX * NY * NZ
    weights_pad = jnp.pad(permittivity, 1)
    potential = start_potential
    norms = []
    charges = []
    for iteration in range(ITERS):
        center, residual, diagonal, induced = relax(jnp.pad(potential, 1), weights_pad, screening, source)
        rms = jnp.sqrt(jnp.sum(residual * residual) / cells + 1e-06)
        norms.append(rms)
        charges.append(jnp.sum(induced) / cells)
        potential = center + 1.0 / (1.0 + rms) * residual / diagonal
    return (potential, jnp.stack(norms), jnp.stack(charges))
```

```python
import functools
import jax
import jax.numpy as jnp
from jax import lax
from jax.experimental import pallas as pl
from jax.experimental.pallas import tpu as pltpu
from jax.sharding import PartitionSpec as P

ITERS = 3
AXES = ("gx", "gy", "gz")
OFF = 8
CHUNK = 32
LOG2E = 1.4426950408889634
F32 = jnp.float32


def harmonic(left, right):
    total = left + right
    return 2.0 * left * right / jnp.where(total > 0, total, 1.0)


def sides_of(size):
    return 0 if size < 2 else 1 if size == 2 else 2


def swaps(size):
    a = [(i, i ^ 1) for i in range(size) if i ^ 1 < size]
    b = [(i, i + 1) for i in range(1, size - 1, 2)]
    return (a, b + [(j, i) for i, j in b])


def after_of(axis):
    odd = lax.rem(lax.axis_index(axis), 2)
    return (1 - odd, odd)


class Plan:
    def __init__(self, mesh):
        self.sizes = [mesh.shape[a] for a in AXES]
        self.count = self.sizes[0] * self.sizes[1] * self.sizes[2]
        self.swaps = [(d, s) for d in range(3) for s in range(sides_of(self.sizes[d]))]

    def exchange(self, faces):
        out = []
        for (d, s), face in zip(self.swaps, faces):
            out.append(lax.ppermute(face, AXES[d], swaps(self.sizes[d])[s]))
        return out

    def face_shapes(self, shape, lead=()):
        nx, ny, nz = shape
        kinds = ((ny, nz), (nx, 1, nz), (nx, ny))
        return [lead + kinds[d] for d, _ in self.swaps]


def vmem(shape):
    return pltpu.VMEM(tuple(shape), F32)


def call(kernel, out_shapes, args, out_specs=None, aliases=None, cost=(0, 0), name=None):
    vm = pl.BlockSpec(memory_space=pltpu.VMEM)
    return pl.pallas_call(
        kernel,
        out_shape=out_shapes,
        in_specs=[vm] * len(args),
        out_specs=out_specs or [vm] * len(out_shapes),
        input_output_aliases=aliases or {},
        compiler_params=pltpu.CompilerParams(vmem_limit_bytes=16 * 2**20),
        cost_estimate=pl.CostEstimate(flops=cost[0], bytes_accessed=cost[1], transcendentals=0),
        name=name,
    )(*args)


def faces_kernel(plan, phi, eps, *outs):
    nx, ny, nz = phi.shape
    z_faces = []
    for (d, s), out in zip(plan.swaps, outs):
        after = after_of(AXES[d])[s]
        for k, ref in enumerate((phi, eps)):
            if d == 0:
                out[k] = ref[after * (nx - 1)]
            elif d == 1:
                out[k] = ref[:, pl.ds(after * (ny - 1), 1), :]
        if d == 2:
            z_faces.append((after, out))
    if z_faces:
        for k, ref in enumerate((phi, eps)):
            for x in range(nx):
                flipped = ref[x].T
                first, last = flipped[0:1], flipped[nz - 1 : nz]
                for after, out in z_faces:
                    out[k, x : x + 1, :] = jnp.where(after == 1, last, first)


def weights_kernel(phi, eps, pad, wx, wy, wz):
    nx, ny, nz = phi.shape
    lane = lax.broadcasted_iota(jnp.int32, (CHUNK, nz), 1)
    zero = jnp.zeros((ny, nz), F32)
    pad[0] = jnp.zeros(pad.shape[1:], F32)
    pad[nx + 1] = jnp.zeros(pad.shape[1:], F32)
    wx[0] = zero
    wx[nx] = zero

    def plane(x, carry):
        edge = jnp.zeros((OFF, nz), F32)
        pad[x + 1, 0:OFF] = edge
        pad[x + 1, OFF + ny : 2 * OFF + ny] = edge
        wy[x, 0:OFF] = edge
        wy[x, OFF + ny : 2 * OFF + ny] = edge
        for y in range(0, ny, CHUNK):
            here = eps[x, y : y + CHUNK]
            pad[x + 1, OFF + y : OFF + y + CHUNK] = phi[x, y : y + CHUNK]
            right = harmonic(here, pltpu.roll(here, nz - 1, 1))
            wz[x, y : y + CHUNK] = jnp.where(lane == nz - 1, 0.0, right)
            if y + CHUNK < ny:
                wy[x, OFF + y : OFF + y + CHUNK] = harmonic(here, eps[x, y + 1 : y + 1 + CHUNK])
            else:
                wy[x, OFF + y : OFF + y + CHUNK - 1] = harmonic(
                    eps[x, y : y + CHUNK - 1], eps[x, y + 1 : y + CHUNK]
                )
                wy[x, OFF + ny - 1 : OFF + ny] = jnp.zeros((1, nz), F32)
        return carry

    lax.fori_loop(0, nx, plane, 0)

    def deep(x, carry):
        for y in range(0, ny, CHUNK):
            wx[x + 1, y : y + CHUNK] = harmonic(eps[x, y : y + CHUNK], eps[x + 1, y : y + CHUNK])
        return carry

    lax.fori_loop(0, nx - 1, deep, 0)


def spread(scratch, before, after):
    nz = scratch.shape[0]
    nx = before.shape[0]
    for x in range(nx):
        scratch[2 * x : 2 * x + 1] = before[x : x + 1]
        row = (2 * x - 1) % nz
        scratch[row : row + 1] = after[x : x + 1]
    return scratch[...].T


def sweep(plan, refs, z_flux, z_weight):
    pad, wx, wy, wz, diag, scr, src, d, stats, faces, gt, gw, turn = refs
    nx, ny, nz = d.shape
    lane = lax.broadcasted_iota(jnp.int32, (CHUNK, nz), 1)
    edge = (lane == 0) | (lane == nz - 1)
    first = z_weight is not None
    turn[...] = jnp.zeros(turn.shape, F32)
    gt[...] = spread(turn, *z_flux)
    if first:
        gw[...] = spread(turn, *z_weight)
    z_faces = [
        (after_of("gz")[s], out) for (dim, s), out in zip(plan.swaps, faces) if dim == 2
    ]

    def plane(x, sums):
        squares, charges = sums
        shift = lax.rem(nz - 2 * x, nz)
        for y in range(0, ny, CHUNK):
            rows = pl.ds(y, CHUNK)
            c = pad[x + 1, OFF + y : OFF + y + CHUNK]
            w_xp, w_xm = wx[x + 1, rows], wx[x, rows]
            w_yp = wy[x, OFF + y : OFF + y + CHUNK]
            w_ym = wy[x, OFF - 1 + y : OFF - 1 + y + CHUNK]
            w_z = wz[x, rows]
            f_z = w_z * (c - pltpu.roll(c, nz - 1, 1))
            flux = w_xp * (c - pad[x + 2, OFF + y : OFF + y + CHUNK])
            flux += w_xm * (c - pad[x, OFF + y : OFF + y + CHUNK])
            flux += w_yp * (c - pad[x + 1, OFF + 1 + y : OFF + 1 + y + CHUNK])
            flux += w_ym * (c - pad[x + 1, OFF - 1 + y : OFF - 1 + y + CHUNK])
            flux += f_z - pltpu.roll(f_z, 1, 1)
            flux += jnp.where(edge, pltpu.roll(gt[rows], shift, 1), 0.0)
            if first:
                total = (w_xp + w_xm) + (w_yp + w_ym) + (w_z + pltpu.roll(w_z, 1, 1))
                total += jnp.where(edge, pltpu.roll(gw[rows], shift, 1), 0.0)
                diag[x, rows] = total
            else:
                total = diag[x, rows]
            up = jnp.exp2(c * LOG2E)
            down = jnp.exp2(c * -LOG2E)
            c2 = c * c
            series = c * (1.0 + c2 * (1.0 / 6.0 + c2 * (1.0 / 120.0)))
            s = scr[x, rows]
            charge = s * jnp.where(c2 < 0.0625, series, 0.5 * (up - down))
            res = src[x, rows] - flux - charge
            total = total + s * (0.5 * (up + down))
            d[x, rows] = res / jnp.where(total > 0, total, 1.0)
            squares += jnp.sum((res * res).reshape(CHUNK // 8, 8, nz), axis=0)
            charges += jnp.sum(charge.reshape(CHUNK // 8, 8, nz), axis=0)
        if z_faces:
            flipped = d[x].T
            head, tail = flipped[0:1], flipped[nz - 1 : nz]
            for after, out in z_faces:
                out[pl.ds(x, 1), :] = jnp.where(after == 1, tail, head)
        return (squares, charges)

    none = jnp.zeros((8, nz), F32)
    squares, charges = lax.fori_loop(0, nx, plane, (none, none))
    half = nz // 2
    a = jnp.sum(squares, axis=0, keepdims=True)
    b = jnp.sum(charges, axis=0, keepdims=True)
    a = a + pltpu.roll(a, half, 1)
    b = b + pltpu.roll(b, half, 1)
    low = lax.broadcasted_iota(jnp.int32, (1, nz), 1) < half
    stats[...] = jnp.broadcast_to(jnp.where(low, a, b), stats.shape)
    for (dim, s), out in zip(plan.swaps, faces):
        after = after_of(AXES[dim])[s]
        if dim == 0:
            out[...] = d[after * (nx - 1)]
        elif dim == 1:
            out[...] = d[:, pl.ds(after * (ny - 1), 1), :]


def totals(stats, cells):
    rows, nz = stats.shape
    both = jnp.sum(stats[...], axis=0, keepdims=True)
    low = lax.broadcasted_iota(jnp.int32, (1, nz), 1) < nz // 2
    squares = jnp.sum(jnp.where(low, both, 0.0), axis=1, keepdims=True)
    charges = jnp.sum(jnp.where(low, 0.0, both), axis=1, keepdims=True)
    return jnp.sqrt(squares / cells + 1e-06), charges / cells


def z_pair(plan, values, like):
    zero = jnp.zeros(like, F32)
    if not values:
        return (zero, zero)
    one = after_of("gz")[0] == 1
    other = values[1] if len(values) > 1 else zero
    return (jnp.where(one, other, values[0]), jnp.where(one, values[0], other))


def first_kernel(plan, *refs):
    k = len(plan.swaps)
    sent, got = refs[:k], refs[k : 2 * k]
    _, _, _, wz, scr, src = refs[2 * k : 2 * k + 6]
    pad, wx, wy, diag, d, stats, zs = refs[2 * k + 6 : 2 * k + 13]
    faces = refs[2 * k + 13 : 3 * k + 13]
    gt, gw, turn = refs[3 * k + 13 :]
    nx, ny, nz = d.shape
    fluxes, weights = [], []
    for (dim, s), mine, theirs in zip(plan.swaps, sent, got):
        after = after_of(AXES[dim])[s]
        if dim == 0:
            pad[after * (nx + 1), OFF : OFF + ny] = theirs[0]
            wx[after * nx] = harmonic(mine[1], theirs[1])
        elif dim == 1:
            row = OFF - 1 + after * (ny + 1)
            pad[1 : nx + 1, pl.ds(row, 1), :] = theirs[0]
            wy[:, pl.ds(OFF - 1 + after * ny, 1), :] = harmonic(mine[1], theirs[1])
        else:
            w = harmonic(mine[1], theirs[1])
            zs[3 * s] = mine[0]
            zs[3 * s + 1] = theirs[0]
            zs[3 * s + 2] = w
            weights.append(w)
            fluxes.append(w * (mine[0] - theirs[0]))
    like = (nx, ny)
    sweep(
        plan,
        (pad, wx, wy, wz, diag, scr, src, d, stats, faces, gt, gw, turn),
        z_pair(plan, fluxes, like),
        z_pair(plan, weights, like),
    )


def advance(plan, pad, d, omega):
    nx, ny, nz = d.shape

    def plane(x, carry):
        pad[x + 1, OFF : OFF + ny] += omega * d[x]
        return carry

    lax.fori_loop(0, nx, plane, 0)


def next_kernel(plan, cells, *refs):
    k = len(plan.swaps)
    sent, got = refs[:k], refs[k : 2 * k]
    seen, d_old, _, zs_old, wx, wy, wz, diag, scr, src = refs[2 * k : 2 * k + 10]
    pad, d, stats, zs = refs[2 * k + 10 : 2 * k + 14]
    faces = refs[2 * k + 14 : 3 * k + 14]
    gt, turn = refs[3 * k + 14 :]
    nx, ny, nz = d.shape
    rms, _ = totals(seen, cells)
    omega = 1.0 / (1.0 + rms)
    advance(plan, pad, d_old, omega)
    fluxes = []
    for (dim, s), mine, theirs in zip(plan.swaps, sent, got):
        after = after_of(AXES[dim])[s]
        if dim == 0:
            pad[after * (nx + 1), OFF : OFF + ny] += omega * theirs[...]
        elif dim == 1:
            row = OFF - 1 + after * (ny + 1)
            pad[1 : nx + 1, pl.ds(row, 1), :] += omega[:, None] * theirs[...]
        else:
            own = zs_old[3 * s] + omega * mine[...]
            far = zs_old[3 * s + 1] + omega * theirs[...]
            w = zs_old[3 * s + 2]
            zs[3 * s] = own
            zs[3 * s + 1] = far
            zs[3 * s + 2] = w
            fluxes.append(w * (own - far))
    sweep(
        plan,
        (pad, wx, wy, wz, diag, scr, src, d, stats, faces, gt, None, turn),
        z_pair(plan, fluxes, (nx, ny)),
        None,
    )


def last_kernel(cells, *refs):
    seen = refs[:ITERS]
    pad, d, out, norms, charges = refs[ITERS:]
    nx, ny, nz = d.shape
    for t in range(ITERS):
        rms, charge = totals(seen[t], cells)
        norms[t] = rms[0, 0]
        charges[t] = charge[0, 0]
    omega = 1.0 / (1.0 + rms)

    def plane(x, carry):
        out[x] = pad[x + 1, OFF : OFF + ny] + omega * d[x]
        return carry

    lax.fori_loop(0, nx, plane, 0)


def body(plan, phi, eps, scr, src):
    shape = phi.shape
    nx, ny, nz = shape
    cells = float(nx * ny * nz * plan.count)
    k = len(plan.swaps)
    work = 60 * nx * ny * nz
    cost = (200 * work, 4 * nx * ny * nz)
    padded = (nx + 2, ny + 2 * OFF, nz)

    def gather(stats):
        return lax.all_to_all(stats, AXES, 0, 0, tiled=True)

    def like(refs):
        return [vmem(r.shape) for r in refs]

    sent = call(
        functools.partial(faces_kernel, plan),
        [vmem(s) for s in plan.face_shapes(shape, (2,))],
        (phi, eps),
        cost=cost,
        name="faces",
    )
    got = plan.exchange(sent)
    pad, wx, wy, wz = call(
        weights_kernel,
        [vmem(padded), vmem((nx + 1, ny, nz)), vmem((nx, ny + 2 * OFF, nz)), vmem(shape)],
        (phi, eps),
        cost=cost,
        name="weights",
    )
    z_state = vmem((6, nx, ny))
    face_out = [vmem(s) for s in plan.face_shapes(shape)]
    vm = pl.BlockSpec(memory_space=pltpu.VMEM)

    def sweep_call(kernel, outs, args, aliases, scratch, name):
        return pl.pallas_call(
            kernel,
            out_shape=outs,
            in_specs=[vm] * len(args),
            out_specs=[vm] * len(outs),
            scratch_shapes=scratch,
            input_output_aliases=aliases,
            compiler_params=pltpu.CompilerParams(vmem_limit_bytes=16 * 2**20),
            cost_estimate=pl.CostEstimate(flops=cost[0], bytes_accessed=cost[1], transcendentals=0),
            name=name,
        )(*args)

    stats_shape = vmem((plan.count, nz))
    turned, flat = vmem((nz, ny)), vmem((ny, nz))
    outs = sweep_call(
        functools.partial(first_kernel, plan),
        like((pad, wx, wy)) + [vmem(shape), vmem(shape), stats_shape, z_state] + face_out,
        (*sent, *got, pad, wx, wy, wz, scr, src),
        {2 * k: 0, 2 * k + 1: 1, 2 * k + 2: 2},
        [flat, flat, turned],
        "sweep_0",
    )
    pad, wx, wy, diag, d, stats, zs = outs[:7]
    sent = outs[7:]
    seen = []
    for t in range(1, ITERS):
        got = plan.exchange(sent)
        seen.append(gather(stats))
        outs = sweep_call(
            functools.partial(next_kernel, plan, cells),
            [vmem(padded), vmem(shape), stats_shape, z_state] + (face_out if t < ITERS - 1 else face_out),
            (*sent, *got, seen[-1], d, pad, zs, wx, wy, wz, diag, scr, src),
            {2 * k + 2: 0},
            [flat, turned],
            f"sweep_{t}",
        )
        pad, d, stats, zs = outs[:4]
        sent = outs[4:]
    seen.append(gather(stats))
    sm = pl.BlockSpec(memory_space=pltpu.SMEM)
    small = jax.ShapeDtypeStruct((ITERS,), F32)
    return call(
        functools.partial(last_kernel, cells),
        [jax.ShapeDtypeStruct(shape, F32), small, small],
        (*seen, pad, d),
        out_specs=[vm, sm, sm],
        cost=cost,
        name="finish",
    )


def solution(mesh):
    block = P(*AXES)
    return jax.shard_map(
        functools.partial(body, Plan(mesh)),
        mesh=mesh,
        in_specs=(block,) * 4,
        out_specs=(block, P(), P()),
        check_vma=False,
    )
```

```python
import functools
import jax
import jax.numpy as jnp
from jax import lax
from jax.experimental import pallas as pl
from jax.experimental.pallas import tpu as pltpu
from jax.sharding import PartitionSpec as P


ITERS = 3
AXES = ("gx", "gy", "gz")
OFF = 8
CHUNK = 32
LOG2E = 1.4426950408889634
F32 = jnp.float32


def harmonic(left, right):
    total = left + right
    return 2.0 * left * right / jnp.where(total > 0, total, 1.0)


def sides_of(size):
    return 0 if size < 2 else 1 if size == 2 else 2


def swaps(size):
    a = [(i, i ^ 1) for i in range(size) if i ^ 1 < size]
    b = [(i, i + 1) for i in range(1, size - 1, 2)]
    return (a, b + [(j, i) for i, j in b])


def after_of(axis):
    odd = lax.rem(lax.axis_index(axis), 2)
    return (1 - odd, odd)


class Plan:
    def __init__(self, mesh):
        self.sizes = [mesh.shape[a] for a in AXES]
        self.count = self.sizes[0] * self.sizes[1] * self.sizes[2]
        self.swaps = [(d, s) for d in range(3) for s in range(sides_of(self.sizes[d]))]

    def exchange(self, faces):
        out = []
        for (d, s), face in zip(self.swaps, faces):
            out.append(lax.ppermute(face, AXES[d], swaps(self.sizes[d])[s]))
        return out

    def face_shapes(self, shape, lead=()):
        nx, ny, nz = shape
        kinds = ((ny, nz), (nx, 1, nz), (nx, ny))
        return [lead + kinds[d] for d, _ in self.swaps]


def vmem(shape):
    return pltpu.VMEM(tuple(shape), F32)


def call(kernel, out_shapes, args, out_specs=None, aliases=None, cost=(0, 0)):
    vm = pl.BlockSpec(memory_space=pltpu.VMEM)
    return pl.pallas_call(
        kernel,
        out_shape=out_shapes,
        in_specs=[vm] * len(args),
        out_specs=out_specs or [vm] * len(out_shapes),
        input_output_aliases=aliases or {},
        compiler_params=pltpu.CompilerParams(vmem_limit_bytes=16 * 2**20),
        cost_estimate=pl.CostEstimate(flops=cost[0], bytes_accessed=cost[1], transcendentals=0),
    )(*args)


def faces_kernel(plan, phi, eps, *outs):
    nx, ny, nz = phi.shape
    z_faces = []
    for (d, s), out in zip(plan.swaps, outs):
        after = after_of(AXES[d])[s]
        for k, ref in enumerate((phi, eps)):
            if d == 0:
                out[k] = ref[after * (nx - 1)]
            elif d == 1:
                out[k] = ref[:, pl.ds(after * (ny - 1), 1), :]
        if d == 2:
            z_faces.append((after, out))
    if z_faces:
        for k, ref in enumerate((phi, eps)):
            for x in range(nx):
                flipped = ref[x].T
                first, last = flipped[0:1], flipped[nz - 1 : nz]
                for after, out in z_faces:
                    out[k, x : x + 1, :] = jnp.where(after == 1, last, first)


def weights_kernel(phi, eps, pad, wx, wy, wz):
    nx, ny, nz = phi.shape
    lane = lax.broadcasted_iota(jnp.int32, (CHUNK, nz), 1)
    zero = jnp.zeros((ny, nz), F32)
    pad[0] = jnp.zeros(pad.shape[1:], F32)
    pad[nx + 1] = jnp.zeros(pad.shape[1:], F32)
    wx[0] = zero
    wx[nx] = zero

    def plane(x, carry):
        edge = jnp.zeros((OFF, nz), F32)
        pad[x + 1, 0:OFF] = edge
        pad[x + 1, OFF + ny : 2 * OFF + ny] = edge
        wy[x, 0:OFF] = edge
        wy[x, OFF + ny : 2 * OFF + ny] = edge
        for y in range(0, ny, CHUNK):
            here = eps[x, y : y + CHUNK]
            pad[x + 1, OFF + y : OFF + y + CHUNK] = phi[x, y : y + CHUNK]
            right = harmonic(here, pltpu.roll(here, nz - 1, 1))
            wz[x, y : y + CHUNK] = jnp.where(lane == nz - 1, 0.0, right)
            if y + CHUNK < ny:
                wy[x, OFF + y : OFF + y + CHUNK] = harmonic(here, eps[x, y + 1 : y + 1 + CHUNK])
            else:
                wy[x, OFF + y : OFF + y + CHUNK - 1] = harmonic(
                    eps[x, y : y + CHUNK - 1], eps[x, y + 1 : y + CHUNK]
                )
                wy[x, OFF + ny - 1 : OFF + ny] = jnp.zeros((1, nz), F32)
        return carry

    lax.fori_loop(0, nx, plane, 0)

    def deep(x, carry):
        for y in range(0, ny, CHUNK):
            wx[x + 1, y : y + CHUNK] = harmonic(eps[x, y : y + CHUNK], eps[x + 1, y : y + CHUNK])
        return carry

    lax.fori_loop(0, nx - 1, deep, 0)


def spread(scratch, before, after):
    nz = scratch.shape[0]
    nx = before.shape[0]
    for x in range(nx):
        scratch[2 * x : 2 * x + 1] = before[x : x + 1]
        row = (2 * x - 1) % nz
        scratch[row : row + 1] = after[x : x + 1]
    return scratch[...].T


def sweep(plan, refs, z_flux, z_weight):
    pad, wx, wy, wz, diag, scr, src, d, stats, faces, gt, gw, turn = refs
    nx, ny, nz = d.shape
    lane = lax.broadcasted_iota(jnp.int32, (CHUNK, nz), 1)
    edge = (lane == 0) | (lane == nz - 1)
    first = z_weight is not None
    turn[...] = jnp.zeros(turn.shape, F32)
    gt[...] = spread(turn, *z_flux)
    if first:
        gw[...] = spread(turn, *z_weight)
    z_faces = [
        (after_of("gz")[s], out) for (dim, s), out in zip(plan.swaps, faces) if dim == 2
    ]

    def plane(x, sums):
        squares, charges = sums
        shift = lax.rem(nz - 2 * x, nz)
        for y in range(0, ny, CHUNK):
            rows = pl.ds(y, CHUNK)
            c = pad[x + 1, OFF + y : OFF + y + CHUNK]
            w_xp, w_xm = wx[x + 1, rows], wx[x, rows]
            w_yp = wy[x, OFF + y : OFF + y + CHUNK]
            w_ym = wy[x, OFF - 1 + y : OFF - 1 + y + CHUNK]
            w_z = wz[x, rows]
            f_z = w_z * (c - pltpu.roll(c, nz - 1, 1))
            flux = w_xp * (c - pad[x + 2, OFF + y : OFF + y + CHUNK])
            flux += w_xm * (c - pad[x, OFF + y : OFF + y + CHUNK])
            flux += w_yp * (c - pad[x + 1, OFF + 1 + y : OFF + 1 + y + CHUNK])
            flux += w_ym * (c - pad[x + 1, OFF - 1 + y : OFF - 1 + y + CHUNK])
            flux += f_z - pltpu.roll(f_z, 1, 1)
            flux += jnp.where(edge, pltpu.roll(gt[rows], shift, 1), 0.0)
            if first:
                total = (w_xp + w_xm) + (w_yp + w_ym) + (w_z + pltpu.roll(w_z, 1, 1))
                total += jnp.where(edge, pltpu.roll(gw[rows], shift, 1), 0.0)
                diag[x, rows] = total
            else:
                total = diag[x, rows]
            up = jnp.exp2(c * LOG2E)
            down = jnp.exp2(c * -LOG2E)
            c2 = c * c
            series = c * (1.0 + c2 * (1.0 / 6.0 + c2 * (1.0 / 120.0)))
            s = scr[x, rows]
            charge = s * jnp.where(c2 < 0.0625, series, 0.5 * (up - down))
            res = src[x, rows] - flux - charge
            total = total + s * (0.5 * (up + down))
            d[x, rows] = res / jnp.where(total > 0, total, 1.0)
            squares += jnp.sum((res * res).reshape(CHUNK // 8, 8, nz), axis=0)
            charges += jnp.sum(charge.reshape(CHUNK // 8, 8, nz), axis=0)
        if z_faces:
            flipped = d[x].T
            head, tail = flipped[0:1], flipped[nz - 1 : nz]
            for after, out in z_faces:
                out[pl.ds(x, 1), :] = jnp.where(after == 1, tail, head)
        return (squares, charges)

    none = jnp.zeros((8, nz), F32)
    squares, charges = lax.fori_loop(0, nx, plane, (none, none))
    half = nz // 2
    a = jnp.sum(squares, axis=0, keepdims=True)
    b = jnp.sum(charges, axis=0, keepdims=True)
    a = a + pltpu.roll(a, half, 1)
    b = b + pltpu.roll(b, half, 1)
    low = lax.broadcasted_iota(jnp.int32, (1, nz), 1) < half
    stats[...] = jnp.broadcast_to(jnp.where(low, a, b), stats.shape)
    for (dim, s), out in zip(plan.swaps, faces):
        after = after_of(AXES[dim])[s]
        if dim == 0:
            out[...] = d[after * (nx - 1)]
        elif dim == 1:
            out[...] = d[:, pl.ds(after * (ny - 1), 1), :]


def totals(stats, cells):
    _, nz = stats.shape
    both = jnp.sum(stats[...], axis=0, keepdims=True)
    low = lax.broadcasted_iota(jnp.int32, (1, nz), 1) < nz // 2
    squares = jnp.sum(jnp.where(low, both, 0.0), axis=1, keepdims=True)
    charges = jnp.sum(jnp.where(low, 0.0, both), axis=1, keepdims=True)
    return jnp.sqrt(squares / cells + 1e-06), charges / cells


def z_pair(values, like):
    zero = jnp.zeros(like, F32)
    if not values:
        return (zero, zero)
    one = after_of("gz")[0] == 1
    other = values[1] if len(values) > 1 else zero
    return (jnp.where(one, other, values[0]), jnp.where(one, values[0], other))


def first_kernel(plan, *refs):
    k = len(plan.swaps)
    sent, got = refs[:k], refs[k : 2 * k]
    _, _, _, wz, scr, src = refs[2 * k : 2 * k + 6]
    pad, wx, wy, diag, d, stats, zs = refs[2 * k + 6 : 2 * k + 13]
    faces = refs[2 * k + 13 : 3 * k + 13]
    gt, gw, turn = refs[3 * k + 13 :]
    nx, ny, _ = d.shape
    fluxes, weights = [], []
    for (dim, s), mine, theirs in zip(plan.swaps, sent, got):
        after = after_of(AXES[dim])[s]
        if dim == 0:
            pad[after * (nx + 1), OFF : OFF + ny] = theirs[0]
            wx[after * nx] = harmonic(mine[1], theirs[1])
        elif dim == 1:
            row = OFF - 1 + after * (ny + 1)
            pad[1 : nx + 1, pl.ds(row, 1), :] = theirs[0]
            wy[:, pl.ds(OFF - 1 + after * ny, 1), :] = harmonic(mine[1], theirs[1])
        else:
            w = harmonic(mine[1], theirs[1])
            zs[3 * s] = mine[0]
            zs[3 * s + 1] = theirs[0]
            zs[3 * s + 2] = w
            weights.append(w)
            fluxes.append(w * (mine[0] - theirs[0]))
    like = (nx, ny)
    sweep(
        plan,
        (pad, wx, wy, wz, diag, scr, src, d, stats, faces, gt, gw, turn),
        z_pair(fluxes, like),
        z_pair(weights, like),
    )


def advance(pad, d, omega):
    nx, ny, _ = d.shape

    def plane(x, carry):
        pad[x + 1, OFF : OFF + ny] += omega * d[x]
        return carry

    lax.fori_loop(0, nx, plane, 0)


def next_kernel(plan, cells, *refs):
    k = len(plan.swaps)
    sent, got = refs[:k], refs[k : 2 * k]
    seen, d_old, _, zs_old, wx, wy, wz, diag, scr, src = refs[2 * k : 2 * k + 10]
    pad, d, stats, zs = refs[2 * k + 10 : 2 * k + 14]
    faces = refs[2 * k + 14 : 3 * k + 14]
    gt, turn = refs[3 * k + 14 :]
    nx, ny, _ = d.shape
    rms, _ = totals(seen, cells)
    omega = 1.0 / (1.0 + rms)
    advance(pad, d_old, omega)
    fluxes = []
    for (dim, s), mine, theirs in zip(plan.swaps, sent, got):
        after = after_of(AXES[dim])[s]
        if dim == 0:
            pad[after * (nx + 1), OFF : OFF + ny] += omega * theirs[...]
        elif dim == 1:
            row = OFF - 1 + after * (ny + 1)
            pad[1 : nx + 1, pl.ds(row, 1), :] += omega[:, None] * theirs[...]
        else:
            own = zs_old[3 * s] + omega * mine[...]
            far = zs_old[3 * s + 1] + omega * theirs[...]
            w = zs_old[3 * s + 2]
            zs[3 * s] = own
            zs[3 * s + 1] = far
            zs[3 * s + 2] = w
            fluxes.append(w * (own - far))
    sweep(
        plan,
        (pad, wx, wy, wz, diag, scr, src, d, stats, faces, gt, None, turn),
        z_pair(fluxes, (nx, ny)),
        None,
    )


def last_kernel(cells, *refs):
    seen = refs[:ITERS]
    pad, d, out, norms, charges = refs[ITERS:]
    nx, ny, _ = d.shape
    for t in range(ITERS):
        rms, charge = totals(seen[t], cells)
        norms[t] = rms[0, 0]
        charges[t] = charge[0, 0]
    omega = 1.0 / (1.0 + rms)

    def plane(x, carry):
        out[x] = pad[x + 1, OFF : OFF + ny] + omega * d[x]
        return carry

    lax.fori_loop(0, nx, plane, 0)


def body(plan, phi, eps, scr, src):
    shape = phi.shape
    nx, ny, nz = shape
    cells = float(nx * ny * nz * plan.count)
    k = len(plan.swaps)
    work = 60 * nx * ny * nz
    cost = (200 * work, 4 * nx * ny * nz)
    padded = (nx + 2, ny + 2 * OFF, nz)

    def gather(stats):
        return lax.all_to_all(stats, AXES, 0, 0, tiled=True)

    def like(refs):
        return [vmem(r.shape) for r in refs]

    sent = call(
        functools.partial(faces_kernel, plan),
        [vmem(s) for s in plan.face_shapes(shape, (2,))],
        (phi, eps),
        cost=cost,
    )
    got = plan.exchange(sent)
    pad, wx, wy, wz = call(
        weights_kernel,
        [vmem(padded), vmem((nx + 1, ny, nz)), vmem((nx, ny + 2 * OFF, nz)), vmem(shape)],
        (phi, eps),
        cost=cost,
    )
    z_state = vmem((6, nx, ny))
    face_out = [vmem(s) for s in plan.face_shapes(shape)]
    vm = pl.BlockSpec(memory_space=pltpu.VMEM)

    def sweep_call(kernel, outs, args, aliases, scratch):
        return pl.pallas_call(
            kernel,
            out_shape=outs,
            in_specs=[vm] * len(args),
            out_specs=[vm] * len(outs),
            scratch_shapes=scratch,
            input_output_aliases=aliases,
            compiler_params=pltpu.CompilerParams(vmem_limit_bytes=16 * 2**20),
            cost_estimate=pl.CostEstimate(flops=cost[0], bytes_accessed=cost[1], transcendentals=0),
        )(*args)

    stats_shape = vmem((plan.count, nz))
    turned, flat = vmem((nz, ny)), vmem((ny, nz))
    outs = sweep_call(
        functools.partial(first_kernel, plan),
        like((pad, wx, wy)) + [vmem(shape), vmem(shape), stats_shape, z_state] + face_out,
        (*sent, *got, pad, wx, wy, wz, scr, src),
        {2 * k: 0, 2 * k + 1: 1, 2 * k + 2: 2},
        [flat, flat, turned],
    )
    pad, wx, wy, diag, d, stats, zs = outs[:7]
    sent = outs[7:]
    seen = []
    for _ in range(1, ITERS):
        got = plan.exchange(sent)
        seen.append(gather(stats))
        outs = sweep_call(
            functools.partial(next_kernel, plan, cells),
            [vmem(padded), vmem(shape), stats_shape, z_state] + face_out,
            (*sent, *got, seen[-1], d, pad, zs, wx, wy, wz, diag, scr, src),
            {2 * k + 2: 0},
            [flat, turned],
        )
        pad, d, stats, zs = outs[:4]
        sent = outs[4:]
    seen.append(gather(stats))
    sm = pl.BlockSpec(memory_space=pltpu.SMEM)
    small = jax.ShapeDtypeStruct((ITERS,), F32)
    return call(
        functools.partial(last_kernel, cells),
        [jax.ShapeDtypeStruct(shape, F32), small, small],
        (*seen, pad, d),
        out_specs=[vm, sm, sm],
        cost=cost,
    )


def solution(mesh):
    block = P(*AXES)
    return jax.shard_map(
        functools.partial(body, Plan(mesh)),
        mesh=mesh,
        in_specs=(block,) * 4,
        out_specs=(block, P(), P()),
        check_vma=False,
    )
```

```python
import functools
import jax
import jax.numpy as jnp
from jax import lax
from jax.experimental import pallas as pl
from jax.experimental.pallas import tpu as pltpu
from jax.sharding import PartitionSpec as P


ITERS = 3
AXES = ("gx", "gy", "gz")
OFF = 8
CHUNK = 32
LOG2E = 1.4426950408889634
F32 = jnp.float32


def harmonic(left, right):
    total = left + right
    return 2.0 * left * right / jnp.where(total > 0, total, 1.0)


def sides_of(size):
    return 0 if size < 2 else 1 if size == 2 else 2


def swaps(size):
    a = [(i, i ^ 1) for i in range(size) if i ^ 1 < size]
    b = [(i, i + 1) for i in range(1, size - 1, 2)]
    return (a, b + [(j, i) for i, j in b])


def after_of(axis):
    odd = lax.rem(lax.axis_index(axis), 2)
    return (1 - odd, odd)


class Plan:
    def __init__(self, mesh):
        self.sizes = [mesh.shape[a] for a in AXES]
        self.count = self.sizes[0] * self.sizes[1] * self.sizes[2]
        self.swaps = [(d, s) for d in range(3) for s in range(sides_of(self.sizes[d]))]

    def exchange(self, faces):
        out = []
        for (d, s), face in zip(self.swaps, faces):
            out.append(lax.ppermute(face, AXES[d], swaps(self.sizes[d])[s]))
        return out

    def face_shapes(self, shape, lead=()):
        nx, ny, nz = shape
        kinds = ((ny, nz), (nx, 1, nz), (nx, ny))
        return [lead + kinds[d] for d, _ in self.swaps]


def vmem(shape):
    return pltpu.VMEM(tuple(shape), F32)


def faces_kernel(plan, phi_in, eps_in, *refs):
    outs, (phi, eps, sems) = refs[:-3], refs[-3:]
    copies = [
        pltpu.make_async_copy(phi_in, phi, sems.at[0]),
        pltpu.make_async_copy(eps_in, eps, sems.at[1]),
    ]
    for copy in copies:
        copy.start()
    nx, ny, nz = phi.shape
    z_faces = [(after_of("gz")[s], o) for (d, s), o in zip(plan.swaps, outs) if d == 2]
    for k, ref in enumerate((phi, eps)):
        copies[k].wait()
        for (d, s), out in zip(plan.swaps, outs):
            after = after_of(AXES[d])[s]
            if d == 0:
                out[k] = ref[after * (nx - 1)]
            elif d == 1:
                out[k] = ref[:, pl.ds(after * (ny - 1), 1), :]
        if z_faces:
            for x in range(nx):
                flipped = ref[x].T
                first, last = flipped[0:1], flipped[nz - 1 : nz]
                for after, out in z_faces:
                    out[k, x : x + 1, :] = jnp.where(after == 1, last, first)


def weights_kernel(phi, eps, pad, wx, wy, wz, wz_low):
    nx, ny, nz = phi.shape
    lane = lax.broadcasted_iota(jnp.int32, (CHUNK, nz), 1)
    zero = jnp.zeros((ny, nz), F32)
    pad[0] = jnp.zeros(pad.shape[1:], F32)
    pad[nx + 1] = jnp.zeros(pad.shape[1:], F32)
    wx[0] = zero
    wx[nx] = zero

    def plane(x, carry):
        edge = jnp.zeros((OFF, nz), F32)
        pad[x + 1, 0:OFF] = edge
        pad[x + 1, OFF + ny : 2 * OFF + ny] = edge
        wy[x, 0:OFF] = edge
        wy[x, OFF + ny : 2 * OFF + ny] = edge
        for y in range(0, ny, CHUNK):
            rows = pl.ds(y, CHUNK)
            here = eps[x, rows]
            pad[x + 1, OFF + y : OFF + y + CHUNK] = phi[x, rows]
            high = harmonic(here, pltpu.roll(here, nz - 1, 1))
            low = harmonic(here, pltpu.roll(here, 1, 1))
            wz[x, rows] = jnp.where(lane == nz - 1, 0.0, high)
            wz_low[x, rows] = jnp.where(lane == 0, 0.0, low)
            if y + CHUNK < ny:
                wy[x, OFF + y : OFF + y + CHUNK] = harmonic(here, eps[x, y + 1 : y + 1 + CHUNK])
            else:
                wy[x, OFF + y : OFF + y + CHUNK - 1] = harmonic(
                    eps[x, y : y + CHUNK - 1], eps[x, y + 1 : y + CHUNK]
                )
                wy[x, OFF + ny - 1 : OFF + ny] = jnp.zeros((1, nz), F32)
        return carry

    lax.fori_loop(0, nx, plane, 0)

    def deep(x, carry):
        for y in range(0, ny, CHUNK):
            wx[x + 1, y : y + CHUNK] = harmonic(eps[x, y : y + CHUNK], eps[x + 1, y : y + CHUNK])
        return carry

    lax.fori_loop(0, nx - 1, deep, 0)


def spread(scratch, before, after):
    nz = scratch.shape[0]
    nx = before.shape[0]
    for x in range(nx):
        scratch[2 * x : 2 * x + 1] = before[x : x + 1]
        row = (2 * x - 1) % nz
        scratch[row : row + 1] = after[x : x + 1]
    return scratch[...].T


def sweep(plan, refs, z_flux, z_weight, step):
    pad, wx, wy, wz, wz_low, diag, scr, src, d, stats, faces, scratch = refs
    gt, gw, turn, z_high, z_low, z_rows = scratch
    nx, ny, nz = src.shape
    lane = lax.broadcasted_iota(jnp.int32, (CHUNK, nz), 1)
    edge = (lane == 0) | (lane == nz - 1)
    first = z_weight is not None
    turn[...] = jnp.zeros(turn.shape, F32)
    gt[...] = spread(turn, *z_flux)
    if first:
        gw[...] = spread(turn, *z_weight)
    z_faces = [(after_of("gz")[s], o) for (dim, s), o in zip(plan.swaps, faces) if dim == 2]

    def ready(x):
        for y in range(0, ny, CHUNK):
            rows = pl.ds(y, CHUNK)
            mine = pl.ds(OFF + y, CHUNK)
            if step is None:
                c = pad[x + 1, mine]
            else:
                old, change, omega = step
                c = old[x + 1, mine] + omega * change[x + 1, rows]
                pad[x + 1, mine] = c
            z_high[x, rows] = pltpu.roll(c, nz - 1, 1)
            z_low[x, rows] = pltpu.roll(c, 1, 1)

    def turned(x):
        flipped = d[x + 1].T
        head, tail = flipped[0:1], flipped[nz - 1 : nz]
        for k, (after, _) in enumerate(z_faces):
            z_rows[k, pl.ds(x + 8, 1), :] = jnp.where(after == 1, tail, head)

    def solve(x, sums):
        squares, charges = sums
        shift = lax.rem(nz - 2 * x, nz)
        for y in range(0, ny, CHUNK):
            rows = pl.ds(y, CHUNK)
            c = pad[x + 1, OFF + y : OFF + y + CHUNK]
            w_xp, w_xm = wx[x + 1, rows], wx[x, rows]
            w_yp = wy[x, OFF + y : OFF + y + CHUNK]
            w_ym = wy[x, OFF - 1 + y : OFF - 1 + y + CHUNK]
            w_zp, w_zm = wz[x, rows], wz_low[x, rows]
            flux = w_xp * (c - pad[x + 2, OFF + y : OFF + y + CHUNK])
            flux += w_xm * (c - pad[x, OFF + y : OFF + y + CHUNK])
            flux += w_yp * (c - pad[x + 1, OFF + 1 + y : OFF + 1 + y + CHUNK])
            flux += w_ym * (c - pad[x + 1, OFF - 1 + y : OFF - 1 + y + CHUNK])
            flux += w_zp * (c - z_high[x, rows])
            flux += w_zm * (c - z_low[x, rows])
            flux += jnp.where(edge, pltpu.roll(gt[rows], shift, 1), 0.0)
            if first:
                total = (w_xp + w_xm) + (w_yp + w_ym) + (w_zp + w_zm)
                total += jnp.where(edge, pltpu.roll(gw[rows], shift, 1), 0.0)
                diag[x, rows] = total
            else:
                total = diag[x, rows]
            up = jnp.exp2(c * LOG2E)
            down = jnp.exp2(c * -LOG2E)
            c2 = c * c
            series = c * (1.0 + c2 * (1.0 / 6.0 + c2 * (1.0 / 120.0)))
            s = scr[x, rows]
            charge = s * jnp.where(c2 < 0.0625, series, 0.5 * (up - down))
            res = src[x, rows] - flux - charge
            total = total + s * (0.5 * (up + down))
            d[x + 1, rows] = res / jnp.where(total > 0, total, 1.0)
            squares += jnp.sum((res * res).reshape(CHUNK // 8, 8, nz), axis=0)
            charges += jnp.sum(charge.reshape(CHUNK // 8, 8, nz), axis=0)
        return (squares, charges)

    def full(x, sums):
        if z_faces:
            turned(x - 1)
        ready(x + 2)
        return solve(x, sums)

    def tail(x, sums):
        if z_faces:
            turned(x - 1)
        return solve(x, sums)

    ahead = min(2, nx)
    for x in range(ahead):
        ready(x)
    if z_faces:
        d[0] = jnp.zeros((ny, nz), F32)
    none = jnp.zeros((8, nz), F32)
    sums = lax.fori_loop(0, nx - ahead, full, (none, none))
    squares, charges = lax.fori_loop(nx - ahead, nx, tail, sums)
    half = nz // 2
    a = jnp.sum(squares, axis=0, keepdims=True)
    b = jnp.sum(charges, axis=0, keepdims=True)
    a = a + pltpu.roll(a, half, 1)
    b = b + pltpu.roll(b, half, 1)
    low = lax.broadcasted_iota(jnp.int32, (1, nz), 1) < half
    stats[...] = jnp.broadcast_to(jnp.where(low, a, b), stats.shape)
    if z_faces:
        turned(nx - 1)
        for k, (_, out) in enumerate(z_faces):
            out[...] = z_rows[k, 8 : 8 + nx]
    if faces:
        for (dim, s), out in zip(plan.swaps, faces):
            after = after_of(AXES[dim])[s]
            if dim == 0:
                out[...] = d[1 + after * (nx - 1)]
            elif dim == 1:
                out[...] = d[1 : nx + 1, pl.ds(after * (ny - 1), 1), :]


def totals(stats, cells):
    _, nz = stats.shape
    both = jnp.sum(stats[...], axis=0, keepdims=True)
    low = lax.broadcasted_iota(jnp.int32, (1, nz), 1) < nz // 2
    squares = jnp.sum(jnp.where(low, both, 0.0), axis=1, keepdims=True)
    charges = jnp.sum(jnp.where(low, 0.0, both), axis=1, keepdims=True)
    return jnp.sqrt(squares / cells + 1e-06), charges / cells


def z_pair(values, like):
    zero = jnp.zeros(like, F32)
    if not values:
        return (zero, zero)
    one = after_of("gz")[0] == 1
    other = values[1] if len(values) > 1 else zero
    return (jnp.where(one, other, values[0]), jnp.where(one, values[0], other))


def first_kernel(plan, *refs):
    k = len(plan.swaps)
    sent, got = refs[:k], refs[k : 2 * k]
    _, _, _, wz, wz_low, scr, src = refs[2 * k : 2 * k + 7]
    pad, wx, wy, diag, d, stats, zs = refs[2 * k + 7 : 2 * k + 14]
    faces = refs[2 * k + 14 : 3 * k + 14]
    scratch = refs[3 * k + 14 :]
    nx, ny, _ = src.shape
    fluxes, weights = [], []
    for (dim, s), mine, theirs in zip(plan.swaps, sent, got):
        after = after_of(AXES[dim])[s]
        if dim == 0:
            pad[after * (nx + 1), OFF : OFF + ny] = theirs[0]
            wx[after * nx] = harmonic(mine[1], theirs[1])
        elif dim == 1:
            row = OFF - 1 + after * (ny + 1)
            pad[1 : nx + 1, pl.ds(row, 1), :] = theirs[0]
            wy[:, pl.ds(OFF - 1 + after * ny, 1), :] = harmonic(mine[1], theirs[1])
        else:
            w = harmonic(mine[1], theirs[1])
            zs[3 * s] = mine[0]
            zs[3 * s + 1] = theirs[0]
            zs[3 * s + 2] = w
            weights.append(w)
            fluxes.append(w * (mine[0] - theirs[0]))
    like = (nx, ny)
    sweep(
        plan,
        (pad, wx, wy, wz, wz_low, diag, scr, src, d, stats, faces, scratch),
        z_pair(fluxes, like),
        z_pair(weights, like),
        None,
    )


def next_kernel(plan, cells, final, *refs):
    k = len(plan.swaps)
    sent, got = refs[:k], refs[k : 2 * k]
    seen, d_old, old, zs_old, wx, wy, wz, wz_low, diag, scr, src = refs[2 * k : 2 * k + 11]
    pad, d, stats = refs[2 * k + 11 : 2 * k + 14]
    rest = refs[2 * k + 14 :]
    zs, faces, scratch = (None, (), rest) if final else (rest[0], rest[1 : k + 1], rest[k + 1 :])
    nx, ny, _ = src.shape
    rms, _ = totals(seen, cells)
    omega = 1.0 / (1.0 + rms)
    pad[0, OFF : OFF + ny] = old[0, OFF : OFF + ny]
    pad[nx + 1, OFF : OFF + ny] = old[nx + 1, OFF : OFF + ny]
    for row in (OFF - 1, OFF + ny):
        pad[1 : nx + 1, row : row + 1, :] = old[1 : nx + 1, row : row + 1, :]
    fluxes = []
    for (dim, s), mine, theirs in zip(plan.swaps, sent, got):
        after = after_of(AXES[dim])[s]
        if dim == 0:
            pad[after * (nx + 1), OFF : OFF + ny] += omega * theirs[...]
        elif dim == 1:
            row = OFF - 1 + after * (ny + 1)
            pad[1 : nx + 1, pl.ds(row, 1), :] += omega[:, None] * theirs[...]
        else:
            own = zs_old[3 * s] + omega * mine[...]
            far = zs_old[3 * s + 1] + omega * theirs[...]
            w = zs_old[3 * s + 2]
            if not final:
                zs[3 * s] = own
                zs[3 * s + 1] = far
                zs[3 * s + 2] = w
            fluxes.append(w * (own - far))
    sweep(
        plan,
        (pad, wx, wy, wz, wz_low, diag, scr, src, d, stats, faces, scratch),
        z_pair(fluxes, (nx, ny)),
        None,
        (old, d_old, omega),
    )


def last_kernel(cells, *refs):
    seen = refs[:ITERS]
    pad, d, out, norms, charges = refs[ITERS:]
    nx, ny, _ = out.shape
    for t in range(ITERS):
        rms, charge = totals(seen[t], cells)
        norms[t] = rms[0, 0]
        charges[t] = charge[0, 0]
    omega = 1.0 / (1.0 + rms)

    def plane(x, carry):
        out[x] = pad[x + 1, OFF : OFF + ny] + omega * d[x + 1]
        return carry

    lax.fori_loop(0, nx, plane, 0)


def body(plan, phi, eps, scr, src):
    shape = phi.shape
    nx, ny, nz = shape
    cells = float(nx * ny * nz * plan.count)
    k = len(plan.swaps)
    cost = pl.CostEstimate(flops=12000 * nx * ny * nz, bytes_accessed=4 * nx * ny * nz, transcendentals=0)
    padded = vmem((nx + 2, ny + 2 * OFF, nz))
    block, shifted = vmem(shape), vmem((nx + 1, ny, nz))
    wide_x, wide_y = shifted, vmem((nx, ny + 2 * OFF, nz))
    vm = pl.BlockSpec(memory_space=pltpu.VMEM)

    def call(kernel, outs, args, in_specs=None, out_specs=None, aliases=None, scratch=()):
        return pl.pallas_call(
            kernel,
            out_shape=outs,
            in_specs=in_specs or [vm] * len(args),
            out_specs=out_specs or [vm] * len(outs),
            scratch_shapes=scratch,
            input_output_aliases=aliases or {},
            compiler_params=pltpu.CompilerParams(vmem_limit_bytes=16 * 2**20),
            cost_estimate=cost,
        )(*args)

    def gather(stats):
        return lax.all_to_all(stats, AXES, 0, 0, tiled=True)

    *sent, phi_v, eps_v = call(
        functools.partial(faces_kernel, plan),
        [vmem(s) for s in plan.face_shapes(shape, (2,))] + [block, block],
        (phi, eps),
        in_specs=[pl.BlockSpec(memory_space=pl.ANY)] * 2,
        scratch=[pltpu.SemaphoreType.DMA((2,))],
    )
    got = plan.exchange(sent)
    pad, wx, wy, wz, wz_low = call(
        weights_kernel, [padded, wide_x, wide_y, block, block], (phi_v, eps_v)
    )
    z_state = vmem((6, nx, ny))
    face_out = [vmem(s) for s in plan.face_shapes(shape)]
    stats_shape = vmem((plan.count, nz))
    flat = vmem((ny, nz))
    scratch = [flat, flat, vmem((nz, ny)), block, block, vmem((2, nx + 8, ny))]
    pad, wx, wy, diag, d, stats, zs, *sent = call(
        functools.partial(first_kernel, plan),
        [padded, wide_x, wide_y, block, shifted, stats_shape, z_state] + face_out,
        (*sent, *got, pad, wx, wy, wz, wz_low, scr, src),
        aliases={2 * k: 0, 2 * k + 1: 1, 2 * k + 2: 2},
        scratch=scratch,
    )
    seen = []
    for t in range(1, ITERS):
        final = t == ITERS - 1
        got = plan.exchange(sent)
        seen.append(gather(stats))
        pad, d, stats, *more = call(
            functools.partial(next_kernel, plan, cells, final),
            [padded, shifted, stats_shape] + ([] if final else [z_state] + face_out),
            (*sent, *got, seen[-1], d, pad, zs, wx, wy, wz, wz_low, diag, scr, src),
            scratch=scratch,
        )
        if not final:
            zs, *sent = more
    seen.append(gather(stats))
    sm = pl.BlockSpec(memory_space=pltpu.SMEM)
    small = jax.ShapeDtypeStruct((ITERS,), F32)
    return call(
        functools.partial(last_kernel, cells),
        [jax.ShapeDtypeStruct(shape, F32), small, small],
        (*seen, pad, d),
        out_specs=[vm, sm, sm],
    )


def solution(mesh):
    block = P(*AXES)
    return jax.shard_map(
        functools.partial(body, Plan(mesh)),
        mesh=mesh,
        in_specs=(block,) * 4,
        out_specs=(block, P(), P()),
        check_vma=False,
    )
```

```python
import functools
import jax
import jax.numpy as jnp
from jax import lax
from jax.experimental import pallas as pl
from jax.experimental.pallas import tpu as pltpu
from jax.sharding import PartitionSpec as P


ITERS = 3
AXES = ("gx", "gy", "gz")
OFF = 8
VMEM_BYTES = 67043328
CHUNK = 32
LOG2E = 1.4426950408889634
F32 = jnp.float32


def harmonic(left, right):
    total = left + right
    return 2.0 * left * right / jnp.where(total > 0, total, 1.0)


def sides_of(size):
    return 0 if size < 2 else 1 if size == 2 else 2


def swaps(size):
    a = [(i, i ^ 1) for i in range(size) if i ^ 1 < size]
    b = [(i, i + 1) for i in range(1, size - 1, 2)]
    return (a, b + [(j, i) for i, j in b])


def after_of(axis):
    odd = lax.rem(lax.axis_index(axis), 2)
    return (1 - odd, odd)


class Plan:
    def __init__(self, mesh):
        self.sizes = [mesh.shape[a] for a in AXES]
        self.count = self.sizes[0] * self.sizes[1] * self.sizes[2]
        self.swaps = [(d, s) for d in range(3) for s in range(sides_of(self.sizes[d]))]

    def exchange(self, faces):
        out = []
        for (d, s), face in zip(self.swaps, faces):
            out.append(lax.ppermute(face, AXES[d], swaps(self.sizes[d])[s]))
        return out

    def face_shapes(self, shape, lead=()):
        nx, ny, nz = shape
        kinds = ((ny, nz), (nx, 1, nz), (nx, ny))
        return [lead + kinds[d] for d, _ in self.swaps]


def vmem(shape):
    return pltpu.VMEM(tuple(shape), F32)


def faces_kernel(plan, phi_in, eps_in, *refs):
    outs, (phi, eps, sems) = refs[:-3], refs[-3:]
    copies = [
        pltpu.make_async_copy(phi_in, phi, sems.at[0]),
        pltpu.make_async_copy(eps_in, eps, sems.at[1]),
    ]
    for copy in copies:
        copy.start()
    nx, ny, nz = phi.shape
    z_faces = [(after_of("gz")[s], o) for (d, s), o in zip(plan.swaps, outs) if d == 2]
    for k, ref in enumerate((phi, eps)):
        copies[k].wait()
        for (d, s), out in zip(plan.swaps, outs):
            after = after_of(AXES[d])[s]
            if d == 0:
                out[k] = ref[after * (nx - 1)]
            elif d == 1:
                out[k] = ref[:, pl.ds(after * (ny - 1), 1), :]
        if z_faces:
            for x in range(nx):
                flipped = ref[x].T
                first, last = flipped[0:1], flipped[nz - 1 : nz]
                for after, out in z_faces:
                    out[k, x : x + 1, :] = jnp.where(after == 1, last, first)


def weights_kernel(phi, eps, pad, wx, wy, wz, wz_low):
    nx, ny, nz = phi.shape
    lane = lax.broadcasted_iota(jnp.int32, (CHUNK, nz), 1)
    zero = jnp.zeros((ny, nz), F32)
    pad[0] = jnp.zeros(pad.shape[1:], F32)
    pad[nx + 1] = jnp.zeros(pad.shape[1:], F32)
    wx[0] = zero
    wx[nx] = zero

    def plane(x, carry):
        edge = jnp.zeros((OFF, nz), F32)
        pad[x + 1, 0:OFF] = edge
        pad[x + 1, OFF + ny : 2 * OFF + ny] = edge
        wy[x, 0:OFF] = edge
        wy[x, OFF + ny : 2 * OFF + ny] = edge
        for y in range(0, ny, CHUNK):
            rows = pl.ds(y, CHUNK)
            here = eps[x, rows]
            pad[x + 1, OFF + y : OFF + y + CHUNK] = phi[x, rows]
            high = harmonic(here, pltpu.roll(here, nz - 1, 1))
            low = harmonic(here, pltpu.roll(here, 1, 1))
            wz[x, rows] = jnp.where(lane == nz - 1, 0.0, high)
            wz_low[x, rows] = jnp.where(lane == 0, 0.0, low)
            if y + CHUNK < ny:
                wy[x, OFF + y : OFF + y + CHUNK] = harmonic(here, eps[x, y + 1 : y + 1 + CHUNK])
            else:
                wy[x, OFF + y : OFF + y + CHUNK - 1] = harmonic(
                    eps[x, y : y + CHUNK - 1], eps[x, y + 1 : y + CHUNK]
                )
                wy[x, OFF + ny - 1 : OFF + ny] = jnp.zeros((1, nz), F32)
        return carry

    lax.fori_loop(0, nx, plane, 0)

    def deep(x, carry):
        for y in range(0, ny, CHUNK):
            wx[x + 1, y : y + CHUNK] = harmonic(eps[x, y : y + CHUNK], eps[x + 1, y : y + CHUNK])
        return carry

    lax.fori_loop(0, nx - 1, deep, 0)


def spread(scratch, before, after):
    nz = scratch.shape[0]
    nx = before.shape[0]
    for x in range(nx):
        scratch[2 * x : 2 * x + 1] = before[x : x + 1]
        row = (2 * x - 1) % nz
        scratch[row : row + 1] = after[x : x + 1]
    return scratch[...].T


def sweep(plan, refs, z_flux, z_weight, step):
    pad, wx, wy, wz, wz_low, diag, scr, src, d, stats, faces, scratch = refs
    gt, gw, turn, z_high, z_low, z_rows = scratch
    nx, ny, nz = src.shape
    lane = lax.broadcasted_iota(jnp.int32, (CHUNK, nz), 1)
    edge = (lane == 0) | (lane == nz - 1)
    first = z_weight is not None
    turn[...] = jnp.zeros(turn.shape, F32)
    gt[...] = spread(turn, *z_flux)
    if first:
        gw[...] = spread(turn, *z_weight)
    z_faces = [(after_of("gz")[s], o) for (dim, s), o in zip(plan.swaps, faces) if dim == 2]

    def ready(x):
        for y in range(0, ny, CHUNK):
            rows = pl.ds(y, CHUNK)
            mine = pl.ds(OFF + y, CHUNK)
            if step is None:
                c = pad[x + 1, mine]
            else:
                old, change, omega = step
                c = old[x + 1, mine] + omega * change[x + 1, rows]
                pad[x + 1, mine] = c
            z_high[x, rows] = pltpu.roll(c, nz - 1, 1)
            z_low[x, rows] = pltpu.roll(c, 1, 1)

    def turned(x):
        flipped = d[x + 1].T
        head, tail = flipped[0:1], flipped[nz - 1 : nz]
        for k, (after, _) in enumerate(z_faces):
            z_rows[k, pl.ds(x + 8, 1), :] = jnp.where(after == 1, tail, head)

    def solve(x, sums):
        squares, charges = sums
        shift = lax.rem(nz - 2 * x, nz)
        for y in range(0, ny, CHUNK):
            rows = pl.ds(y, CHUNK)
            c = pad[x + 1, OFF + y : OFF + y + CHUNK]
            w_xp, w_xm = wx[x + 1, rows], wx[x, rows]
            w_yp = wy[x, OFF + y : OFF + y + CHUNK]
            w_ym = wy[x, OFF - 1 + y : OFF - 1 + y + CHUNK]
            w_zp, w_zm = wz[x, rows], wz_low[x, rows]
            flux = w_xp * (c - pad[x + 2, OFF + y : OFF + y + CHUNK])
            flux += w_xm * (c - pad[x, OFF + y : OFF + y + CHUNK])
            flux += w_yp * (c - pad[x + 1, OFF + 1 + y : OFF + 1 + y + CHUNK])
            flux += w_ym * (c - pad[x + 1, OFF - 1 + y : OFF - 1 + y + CHUNK])
            flux += w_zp * (c - z_high[x, rows])
            flux += w_zm * (c - z_low[x, rows])
            flux += jnp.where(edge, pltpu.roll(gt[rows], shift, 1), 0.0)
            if first:
                total = (w_xp + w_xm) + (w_yp + w_ym) + (w_zp + w_zm)
                total += jnp.where(edge, pltpu.roll(gw[rows], shift, 1), 0.0)
                diag[x, rows] = total
            else:
                total = diag[x, rows]
            up = jnp.exp2(c * LOG2E)
            down = jnp.exp2(c * -LOG2E)
            c2 = c * c
            series = c * (1.0 + c2 * (1.0 / 6.0 + c2 * (1.0 / 120.0)))
            s = scr[x, rows]
            charge = s * jnp.where(c2 < 0.0625, series, 0.5 * (up - down))
            res = src[x, rows] - flux - charge
            total = total + s * (0.5 * (up + down))
            d[x + 1, rows] = res / jnp.where(total > 0, total, 1.0)
            squares += jnp.sum((res * res).reshape(CHUNK // 8, 8, nz), axis=0)
            charges += jnp.sum(charge.reshape(CHUNK // 8, 8, nz), axis=0)
        return (squares, charges)

    def full(x, sums):
        if z_faces:
            turned(x - 1)
        ready(x + 2)
        return solve(x, sums)

    def tail(x, sums):
        if z_faces:
            turned(x - 1)
        return solve(x, sums)

    ahead = min(2, nx)
    for x in range(ahead):
        ready(x)
    if z_faces:
        d[0] = jnp.zeros((ny, nz), F32)
    none = jnp.zeros((8, nz), F32)
    sums = lax.fori_loop(0, nx - ahead, full, (none, none))
    squares, charges = lax.fori_loop(nx - ahead, nx, tail, sums)
    half = nz // 2
    a = jnp.sum(squares, axis=0, keepdims=True)
    b = jnp.sum(charges, axis=0, keepdims=True)
    a = a + pltpu.roll(a, half, 1)
    b = b + pltpu.roll(b, half, 1)
    low = lax.broadcasted_iota(jnp.int32, (1, nz), 1) < half
    stats[...] = jnp.broadcast_to(jnp.where(low, a, b), stats.shape)
    if z_faces:
        turned(nx - 1)
        for k, (_, out) in enumerate(z_faces):
            out[...] = z_rows[k, 8 : 8 + nx]
    if faces:
        for (dim, s), out in zip(plan.swaps, faces):
            after = after_of(AXES[dim])[s]
            if dim == 0:
                out[...] = d[1 + after * (nx - 1)]
            elif dim == 1:
                out[...] = d[1 : nx + 1, pl.ds(after * (ny - 1), 1), :]


def totals(stats, cells):
    _, nz = stats.shape
    both = jnp.sum(stats[...], axis=0, keepdims=True)
    low = lax.broadcasted_iota(jnp.int32, (1, nz), 1) < nz // 2
    squares = jnp.sum(jnp.where(low, both, 0.0), axis=1, keepdims=True)
    charges = jnp.sum(jnp.where(low, 0.0, both), axis=1, keepdims=True)
    return jnp.sqrt(squares / cells + 1e-06), charges / cells


def z_pair(values, like):
    zero = jnp.zeros(like, F32)
    if not values:
        return (zero, zero)
    one = after_of("gz")[0] == 1
    other = values[1] if len(values) > 1 else zero
    return (jnp.where(one, other, values[0]), jnp.where(one, values[0], other))


def first_kernel(plan, *refs):
    k = len(plan.swaps)
    sent, got = refs[:k], refs[k : 2 * k]
    _, _, _, wz, wz_low, scr, src = refs[2 * k : 2 * k + 7]
    pad, wx, wy, diag, d, stats, zs = refs[2 * k + 7 : 2 * k + 14]
    faces = refs[2 * k + 14 : 3 * k + 14]
    scratch = refs[3 * k + 14 :]
    nx, ny, _ = src.shape
    fluxes, weights = [], []
    for (dim, s), mine, theirs in zip(plan.swaps, sent, got):
        after = after_of(AXES[dim])[s]
        if dim == 0:
            pad[after * (nx + 1), OFF : OFF + ny] = theirs[0]
            wx[after * nx] = harmonic(mine[1], theirs[1])
        elif dim == 1:
            row = OFF - 1 + after * (ny + 1)
            pad[1 : nx + 1, pl.ds(row, 1), :] = theirs[0]
            wy[:, pl.ds(OFF - 1 + after * ny, 1), :] = harmonic(mine[1], theirs[1])
        else:
            w = harmonic(mine[1], theirs[1])
            zs[3 * s] = mine[0]
            zs[3 * s + 1] = theirs[0]
            zs[3 * s + 2] = w
            weights.append(w)
            fluxes.append(w * (mine[0] - theirs[0]))
    like = (nx, ny)
    sweep(
        plan,
        (pad, wx, wy, wz, wz_low, diag, scr, src, d, stats, faces, scratch),
        z_pair(fluxes, like),
        z_pair(weights, like),
        None,
    )


def next_kernel(plan, cells, final, *refs):
    k = len(plan.swaps)
    sent, got = refs[:k], refs[k : 2 * k]
    seen, d_old, old, zs_old, wx, wy, wz, wz_low, diag, scr, src = refs[2 * k : 2 * k + 11]
    pad, d, stats = refs[2 * k + 11 : 2 * k + 14]
    rest = refs[2 * k + 14 :]
    zs, faces, scratch = (None, (), rest) if final else (rest[0], rest[1 : k + 1], rest[k + 1 :])
    nx, ny, _ = src.shape
    rms, _ = totals(seen, cells)
    omega = 1.0 / (1.0 + rms)
    pad[0, OFF : OFF + ny] = old[0, OFF : OFF + ny]
    pad[nx + 1, OFF : OFF + ny] = old[nx + 1, OFF : OFF + ny]
    for row in (OFF - 1, OFF + ny):
        pad[1 : nx + 1, row : row + 1, :] = old[1 : nx + 1, row : row + 1, :]
    fluxes = []
    for (dim, s), mine, theirs in zip(plan.swaps, sent, got):
        after = after_of(AXES[dim])[s]
        if dim == 0:
            pad[after * (nx + 1), OFF : OFF + ny] += omega * theirs[...]
        elif dim == 1:
            row = OFF - 1 + after * (ny + 1)
            pad[1 : nx + 1, pl.ds(row, 1), :] += omega[:, None] * theirs[...]
        else:
            own = zs_old[3 * s] + omega * mine[...]
            far = zs_old[3 * s + 1] + omega * theirs[...]
            w = zs_old[3 * s + 2]
            if not final:
                zs[3 * s] = own
                zs[3 * s + 1] = far
                zs[3 * s + 2] = w
            fluxes.append(w * (own - far))
    sweep(
        plan,
        (pad, wx, wy, wz, wz_low, diag, scr, src, d, stats, faces, scratch),
        z_pair(fluxes, (nx, ny)),
        None,
        (old, d_old, omega),
    )


def last_kernel(cells, *refs):
    seen = refs[:ITERS]
    pad, d, out, norms, charges = refs[ITERS:]
    nx, ny, _ = out.shape
    for t in range(ITERS):
        rms, charge = totals(seen[t], cells)
        norms[t] = rms[0, 0]
        charges[t] = charge[0, 0]
    omega = 1.0 / (1.0 + rms)

    def plane(x, carry):
        out[x] = pad[x + 1, OFF : OFF + ny] + omega * d[x + 1]
        return carry

    lax.fori_loop(0, nx, plane, 0)


def body(plan, phi, eps, scr, src):
    shape = phi.shape
    nx, ny, nz = shape
    cells = float(nx * ny * nz * plan.count)
    k = len(plan.swaps)
    cost = pl.CostEstimate(flops=12000 * nx * ny * nz, bytes_accessed=4 * nx * ny * nz, transcendentals=0)
    padded = vmem((nx + 2, ny + 2 * OFF, nz))
    block, shifted = vmem(shape), vmem((nx + 1, ny, nz))
    wide_x, wide_y = shifted, vmem((nx, ny + 2 * OFF, nz))
    vm = pl.BlockSpec(memory_space=pltpu.VMEM)

    def call(kernel, outs, args, in_specs=None, out_specs=None, aliases=None, scratch=(), room=16 * 2**20):
        return pl.pallas_call(
            kernel,
            out_shape=outs,
            in_specs=in_specs or [vm] * len(args),
            out_specs=out_specs or [vm] * len(outs),
            scratch_shapes=scratch,
            input_output_aliases=aliases or {},
            compiler_params=pltpu.CompilerParams(vmem_limit_bytes=room),
            cost_estimate=cost,
        )(*args)

    def gather(stats):
        return lax.all_to_all(stats, AXES, 0, 0, tiled=True)

    *sent, phi_v, eps_v = call(
        functools.partial(faces_kernel, plan),
        [vmem(s) for s in plan.face_shapes(shape, (2,))] + [block, block],
        (phi, eps),
        in_specs=[pl.BlockSpec(memory_space=pltpu.HBM)] * 2,
        scratch=[pltpu.SemaphoreType.DMA((2,))],
        room=VMEM_BYTES - 4 * (2 * nx * ny * nz + 8 * (ny * nz + nx * nz + nx * ny)) - 2**19,
    )
    got = plan.exchange(sent)
    pad, wx, wy, wz, wz_low = call(
        weights_kernel, [padded, wide_x, wide_y, block, block], (phi_v, eps_v)
    )
    z_state = vmem((6, nx, ny))
    face_out = [vmem(s) for s in plan.face_shapes(shape)]
    stats_shape = vmem((plan.count, nz))
    flat = vmem((ny, nz))
    scratch = [flat, flat, vmem((nz, ny)), block, block, vmem((2, nx + 8, ny))]
    pad, wx, wy, diag, d, stats, zs, *sent = call(
        functools.partial(first_kernel, plan),
        [padded, wide_x, wide_y, block, shifted, stats_shape, z_state] + face_out,
        (*sent, *got, pad, wx, wy, wz, wz_low, scr, src),
        aliases={2 * k: 0, 2 * k + 1: 1, 2 * k + 2: 2},
        scratch=scratch,
    )
    seen = []
    for t in range(1, ITERS):
        final = t == ITERS - 1
        got = plan.exchange(sent)
        seen.append(gather(stats))
        pad, d, stats, *more = call(
            functools.partial(next_kernel, plan, cells, final),
            [padded, shifted, stats_shape] + ([] if final else [z_state] + face_out),
            (*sent, *got, seen[-1], d, pad, zs, wx, wy, wz, wz_low, diag, scr, src),
            scratch=scratch,
        )
        if not final:
            zs, *sent = more
    seen.append(gather(stats))
    sm = pl.BlockSpec(memory_space=pltpu.SMEM)
    small = jax.ShapeDtypeStruct((ITERS,), F32)
    return call(
        functools.partial(last_kernel, cells),
        [jax.ShapeDtypeStruct(shape, F32), small, small],
        (*seen, pad, d),
        out_specs=[vm, sm, sm],
    )


def solution(mesh):
    block = P(*AXES)
    return jax.shard_map(
        functools.partial(body, Plan(mesh)),
        mesh=mesh,
        in_specs=(block,) * 4,
        out_specs=(block, P(), P()),
        check_vma=False,
    )
```
